32 devices in a mesh: row: 4 (over y, x), col: 8 (over z, core).
Axes of the slice: x: 2, y: 2, z: 4, core: 2. Of those that a mesh axis runs over, the one named last changes fastest.
Arguments:
- gate_weight: bfloat16 [4608, 36864], P('row', 'col'), may hold values from -8.838835 to 8.838835
- up_weight: bfloat16 [4608, 36864], P('row', 'col'), may hold values from -8.838835 to 8.838835
- routes: int32 [2, 4], replicated, may hold values from 0 to 3, each once within a row
Outputs:
- gate_serving: bfloat16 [4608, 36864], P('col', 'row')
- up_serving: bfloat16 [4608, 36864], P('col', 'row')
- scales: float32 [2, 36864], P(None, 'row')
The draws below stay inside these ranges and needn't reach their ends.
Inputs may be any that keep to these rules, and one draw needn't show every extreme that they name: Each row of routes names every serving rank's piece once.
All inputs are finite; a program needn't handle non-finite values. Where the reference program divides by a largest or mean magnitude, that divisor is 1e-20 or more.
Results may differ from the reference program's by a relative error of at most 0.001.
Values may be sent and summed in bfloat16 or wider, within the bound.
A program may use at most 128 MiB of HBM per device.

```python
import math
import jax
import jax.numpy as jnp

D = 4608
FF = 36864
SERVE_TP = 4
N_ROW = 4
N_COL = 8


def scaled_weight(key, salt):
    base_key = jax.random.fold_in(key, salt)
    first, second, third = jax.random.split(base_key, 3)
    row_scale = jnp.exp(jax.random.uniform(first, (D, 1), jnp.float32, 0.0, math.log(10.0)))
    col_scale = jnp.exp(jax.random.uniform(second, (1, FF), jnp.float32, 0.0, math.log(10.0)))
    noise = jnp.clip(jax.random.normal(third, (D, FF), jnp.float32), -6.0, 6.0)
    values = noise * row_scale * col_scale / math.sqrt(D)
    return values.astype(jnp.bfloat16)


def draw_gate_weight(key, part):
    return scaled_weight(key, 11)


def draw_up_weight(key, part):
    return scaled_weight(key, 23)


def setup_inputs(seed: int = 0) -> dict:
    keys = jax.random.split(jax.random.key(seed), 4)
    return {
        "gate_weight": draw_gate_weight(jax.random.fold_in(keys[3], 71), 0),
        "up_weight": draw_up_weight(jax.random.fold_in(keys[3], 71), 0),
        "routes": jax.vmap(lambda own: jax.random.permutation(own, SERVE_TP))(jax.random.split(keys[2], 2)).reshape((2, SERVE_TP)).astype(jnp.int32),
    }


EPSILON = 1e-6
LIMIT = 4.0


def convert(weight, order):
    block_len = FF // (N_ROW * N_COL)
    peaks = jnp.max(jnp.abs(weight), axis=0).astype(jnp.float32)
    factor = LIMIT / (peaks + EPSILON)
    quant = (weight.astype(jnp.float32) * factor[None, :]).astype(jnp.bfloat16)
    shaped = quant.reshape(D, N_COL, N_ROW, block_len)
    chosen = jnp.take(shaped, order, axis=2).transpose(0, 2, 1, 3).reshape(D, FF)
    scale_table = ((peaks + EPSILON) / LIMIT).reshape(N_COL, N_ROW, block_len)
    scale_line = jnp.take(scale_table, order, axis=1).transpose(1, 0, 2).reshape(FF)
    return chosen, scale_line


def reference(gate_weight, up_weight, routes):
    gate_serving, gate_scale = convert(gate_weight, routes[0])
    up_serving, up_scale = convert(up_weight, routes[1])
    return gate_serving, up_serving, jnp.stack([gate_scale, up_scale])
```

```python
import functools

import jax
import jax.numpy as jnp
from jax import lax
from jax.experimental import pallas as pl
from jax.experimental.pallas import tpu as pltpu
from jax.sharding import PartitionSpec as P

EPSILON = 1e-06
LIMIT = 4.0
MESH = pl.DeviceIdType.MESH
MOVE_BYTES = 40 * 1024 * 1024
STORE_BYTES = 1024 * 1024
PARTS = 9
LAG = 2


def column_peaks(weight):
    return jnp.max(jnp.abs(weight), axis=0).astype(jnp.float32)


def quantize(weight, peaks):
    factor = LIMIT / (peaks + EPSILON)
    return (weight.astype(jnp.float32) * factor[None, :]).astype(jnp.bfloat16)


def order_pieces(weight, order, pieces):
    height, width = weight.shape
    shaped = weight.reshape(height, pieces, width // pieces)
    return jnp.take(shaped, order, axis=1).reshape(height, width)


def own_piece(peaks, pick, pieces):
    shaped = ((peaks + EPSILON) / LIMIT).reshape(pieces, -1)
    return lax.dynamic_index_in_dim(shaped, pick, 0, keepdims=False)


def exchange(sent):
    sent = lax.all_to_all(sent, "row", split_axis=1, concat_axis=0, tiled=True)
    return lax.all_to_all(sent, "col", split_axis=0, concat_axis=1, tiled=True)


def plain_shards(gate_weight, up_weight, routes):
    pieces = lax.axis_size("row")
    row_index = lax.axis_index("row")
    gate_peaks, up_peaks = lax.pmax((column_peaks(gate_weight), column_peaks(up_weight)), "row")
    gate_serving = exchange(order_pieces(quantize(gate_weight, gate_peaks), routes[0], pieces))
    up_serving = exchange(order_pieces(quantize(up_weight, up_peaks), routes[1], pieces))
    chosen = jnp.take(routes, row_index, axis=1)
    local_scales = jnp.stack(
        [own_piece(gate_peaks, chosen[0], pieces), own_piece(up_peaks, chosen[1], pieces)]
    )
    scales = lax.all_gather(local_scales, "col", axis=1, tiled=True)
    return (gate_serving, up_serving, scales)


def move_kernel(
    n_row, n_col, depth, size, head,
    routes_ref, gate_ref, up_ref, got_ref, scales_ref,
    sent, mid, tops, peak, peak_mid, total, factor, peak_all,
    load, send1, recv1, send2, recv2, psend1, precv1, psend2, precv2,
):
    row, col = lax.axis_index("row"), lax.axis_index("col")
    ratio = n_col // n_row
    height = ratio * depth
    piece = sent.shape[2]
    slots = depth // size
    heads = [(h, q, n) for q, n in head for h in range(ratio)]
    steps = (2 * slots - 1) * ratio
    mine = row * ratio

    def peer_row(s):
        return lax.rem(row + s, n_row)

    def peer_col(s):
        return lax.rem(col + s, n_col)

    def local(ref, target, sem):
        return pltpu.make_async_copy(ref, target, sem)

    def remote(ref, target, send, recv, to_row, to_col):
        return pltpu.make_async_remote_copy(
            src_ref=ref, dst_ref=target, send_sem=send, recv_sem=recv,
            device_id=(to_row, to_col), device_id_type=MESH,
        )

    def fetch(p, h, start, n, index):
        ref = (gate_ref, up_ref)[p]
        for j in range(n_row):
            local(
                ref.at[pl.ds(h * depth + start, n), pl.ds(j * piece, piece)],
                sent.at[j, pl.ds(p * height + h * depth + start, n)],
                load.at[index],
            ).start()

    def fetched(p, h, start, n, index):
        block = sent.at[:, pl.ds(p * height + h * depth + start, n)]
        local(block, block, load.at[index]).wait()

    def rows_of(h, p, start, n):
        src = pl.ds(pl.multiple_of((p * ratio + h) * depth + start, 16), n)
        dst = pl.ds(pl.multiple_of(p * depth + start, 16), n)
        return src, dst

    def start_first(index, h, p, start, n):
        src, dst = rows_of(h, p, start, n)
        for s in range(1, n_row):
            to = peer_row(s)

            @pl.when(mine + h != col)
            def _():
                remote(
                    sent.at[to, src], mid.at[n_row - 1 - s, src],
                    send1.at[s - 1], recv1.at[index, s - 1], to, col,
                ).start()

            @pl.when(mine + h == col)
            def _():
                remote(
                    sent.at[to, src], got_ref.at[col, dst],
                    send1.at[s - 1], recv1.at[index, s - 1], to, col,
                ).start()

    def start_second(s, h, p, start, n, kind):
        src, dst = rows_of(h, p, start, n)
        to = peer_row(n_row - s) * ratio + h
        block = sent.at[row, src] if s == 0 else mid.at[n_row - 1 - s, src]

        @pl.when(to != col)
        def _():
            remote(block, got_ref.at[col, dst], send2.at[s], recv2.at[kind, col], row, to).start()

        if s == 0:
            @pl.when(to == col)
            def _():
                @pl.loop(0, n // 16)
                def _(g):
                    here = pl.ds(pl.multiple_of(src.start + g * 16, 16), 16)
                    there = pl.ds(pl.multiple_of(dst.start + g * 16, 16), 16)
                    got_ref[col, there, :] = sent[row, here, :]

    def forward(index, h, p, start, n, kind):
        src, _ = rows_of(h, p, start, n)
        for s in range(1, n_row):
            block = mid.at[n_row - 1 - s, src]
            local(block, block, recv1.at[index, s - 1]).wait()
            start_second(s, h, p, start, n, kind)

    def pick(p, i, pieces):
        chosen = pieces[0]
        for j in range(1, n_row):
            chosen = jnp.where(routes_ref[p, i] == j, pieces[j], chosen)
        return chosen

    def raise_tops(p, j, block):
        cols = pl.ds(j * piece, piece)
        best = tops[p, :, cols]
        for t in range(block.shape[0] // 16):
            best = jnp.maximum(best, jnp.abs(block[t * 16 : t * 16 + 16]))
        tops[p, :, cols] = best

    def prepare_head(h, start, n):
        @pl.loop(0, n // 16)
        def _(g):
            here = pl.ds(pl.multiple_of(h * depth + start + g * 16, 16), 16)
            pieces = [sent[j, here, :] for j in range(n_row)]
            for j in range(n_row):
                raise_tops(0, j, pieces[j])
            for i in range(n_row):
                sent[i, here, :] = pick(0, i, pieces)

    def scan(p, h, start, n, rows):
        @pl.loop(0, n // rows)
        def _(g):
            here = pl.ds(pl.multiple_of(p * height + h * depth + start + g * rows, 16), rows)
            for j in range(n_row):
                raise_tops(p, j, sent[j, here, :])

    def place(k):
        slot = k // ratio + 1
        return lax.rem(k, ratio), slot // slots, lax.rem(slot, slots) * size

    def prepare(k):
        h, p, start = place(k)
        src, _ = rows_of(h, p, start, size)

        @pl.loop(0, size // 16)
        def _(g):
            here = pl.ds(pl.multiple_of(src.start + g * 16, 16), 16)
            pieces = [sent[j, here, :] for j in range(n_row)]
            for i in range(n_row):
                value = pick(p, i, pieces).astype(jnp.float32)
                sent[i, here, :] = (value * factor[p * n_row + i]).astype(sent.dtype)

    def begin(k):
        h, p, start = place(k)
        start_first(len(heads) + k, h, p, start, size)
        start_second(0, h, p, start, size, 1)

    barrier = pltpu.get_barrier_semaphore()
    for s in range(1, n_row):
        pl.semaphore_signal(barrier, inc=1, device_id=(peer_row(s), col), device_id_type=MESH)
    for s in range(1, n_col):
        pl.semaphore_signal(barrier, inc=1, device_id=(row, peer_col(s)), device_id_type=MESH)

    for h in range(ratio):
        fetch(0, h, 0, size, h)
    blocks = [(p, h) for p in range(2) for h in range(ratio)]
    for b, (p, h) in enumerate(blocks):
        start = size if p == 0 else 0
        fetch(p, h, start, depth - start, ratio + b)
    tops[...] = jnp.zeros_like(tops)

    for h in range(ratio):
        fetched(0, h, 0, size, h)
    for h, q, n in heads:
        prepare_head(h, q, n)

    pl.semaphore_wait(barrier, n_row + n_col - 2)
    for e, (h, q, n) in enumerate(heads):
        start_first(e, h, 0, q, n)
        start_second(0, h, 0, q, n, 0)

    def scan_block(b):
        p, h = blocks[b]
        start = size if p == 0 else 0
        fetched(p, h, start, depth - start, ratio + b)
        scan(p, h, start, depth - start, size if size % 16 == 0 else 16)

    def forward_head(e):
        h, q, n = heads[e]
        forward(e, h, 0, q, n, 0)

    waiting = list(range(len(heads)))
    for b in range(len(blocks)):
        scan_block(b)
        if b >= 1 and waiting:
            forward_head(waiting.pop(0))

    for p in range(2):
        pieces = [
            jnp.max(tops[p, :, pl.ds(j * piece, piece)].astype(jnp.float32), axis=0, keepdims=True)
            for j in range(n_row)
        ]
        for i in range(n_row):
            peak[i, pl.ds(p, 1), :] = pick(p, i, pieces)

    forward_head(waiting.pop(0))

    def peak_first(s):
        return remote(peak, peak_mid.at[s - 1], psend1.at[s - 1], precv1.at[s - 1], peer_row(s), col)

    for s in range(1, n_row):
        peak_first(s).start()
    while waiting:
        forward_head(waiting.pop(0))
    for s in range(1, n_row):
        peak_first(s).wait()
    for i in range(n_row):
        top = peak[i]
        for s in range(1, n_row):
            top = jnp.maximum(top, peak_mid[s - 1, i])
        total[i] = top
        value = LIMIT / (top + EPSILON)
        for p in range(2):
            factor[p * n_row + i] = value[p : p + 1]

    def peak_second(s):
        return remote(
            total.at[row], peak_all.at[col], psend2.at[s - 1], precv2.at[col], row, peer_col(s)
        )

    prepare(0)
    for s in range(1, n_col):
        peak_second(s).start()
    peak_all[col] = total[row]

    @pl.loop(0, steps + LAG)
    def _(k):
        @pl.when(k + 1 < steps)
        def _():
            prepare(k + 1)

        @pl.when(k < steps)
        def _():
            begin(k)

        @pl.when(k >= LAG)
        def _():
            h, p, start = place(k - LAG)
            forward(len(heads) + k - LAG, h, p, start, size, 1)

    for s in range(1, n_col):
        peak_second(s).wait_send()
        other = peer_col(s)
        local(peak_all.at[other], peak_all.at[other], precv2.at[other]).wait()
        block = got_ref.at[other, pl.ds(0, size)]
        local(block, block, recv2.at[0, other]).wait()
    for c in range(n_col):
        base = peak_all[c] + EPSILON
        scales_ref[:, pl.ds(c * piece, piece)] = base / LIMIT
        value = (LIMIT / base)[0:1]

        @pl.loop(0, size // 16)
        def _(g):
            here = pl.ds(pl.multiple_of(g * 16, 16), 16)
            got_ref[c, here, :] = (got_ref[c, here, :].astype(jnp.float32) * value).astype(got_ref.dtype)

    for s in range(1, n_row):
        local(sent.at[0], sent.at[0], send1.at[s - 1]).wait()
    for s in range(n_row):
        kept = peer_row(n_row - s) == col // ratio

        @pl.when(kept)
        def _():
            part = sent.at[0, pl.ds(0, 2 * height - 2 * depth)]
            local(part, part, send2.at[s]).wait()

        @pl.when(jnp.logical_not(kept))
        def _():
            local(sent.at[0], sent.at[0], send2.at[s]).wait()

    for s in range(1, n_col):
        other = peer_col(s)
        block = got_ref.at[other, pl.ds(size, 2 * depth - size)]
        local(block, block, recv2.at[1, other]).wait()


def move_call(gate_weight, up_weight, routes, n_row, n_col, parts):
    height, width = gate_weight.shape
    kind = gate_weight.dtype
    piece = width // n_row
    ratio = n_col // n_row
    depth = height // ratio
    size = depth // parts
    head = [(0, 16), (16, 16), (32, size - 32)]
    copies = len(head) * ratio + (2 * parts - 1) * ratio
    dma = pltpu.SemaphoreType.DMA
    return pl.pallas_call(
        functools.partial(move_kernel, n_row, n_col, depth, size, head),
        out_shape=[
            pltpu.VMEM((n_col, 2 * depth, piece), kind),
            pltpu.VMEM((2, n_col * piece), jnp.float32),
        ],
        in_specs=[
            pl.BlockSpec(memory_space=pltpu.SMEM),
            pl.BlockSpec(memory_space=pl.ANY),
            pl.BlockSpec(memory_space=pl.ANY),
        ],
        out_specs=[
            pl.BlockSpec(memory_space=pltpu.VMEM),
            pl.BlockSpec(memory_space=pltpu.VMEM),
        ],
        scratch_shapes=[
            pltpu.VMEM((n_row, 2 * height, piece), kind),
            pltpu.VMEM((n_row - 1, 2 * height, piece), kind),
            pltpu.VMEM((2, 16, width), kind),
            pltpu.VMEM((n_row, 2, piece), jnp.float32),
            pltpu.VMEM((n_row - 1, n_row, 2, piece), jnp.float32),
            pltpu.VMEM((n_row, 2, piece), jnp.float32),
            pltpu.VMEM((2 * n_row, 1, piece), jnp.float32),
            pltpu.VMEM((n_col, 2, piece), jnp.float32),
            dma((3 * ratio,)),
            dma((n_row - 1,)),
            dma((copies, n_row - 1)),
            dma((n_row,)),
            dma((2, n_col)),
            dma((n_row - 1,)),
            dma((n_row - 1,)),
            dma((n_col - 1,)),
            dma((n_col,)),
        ],
        compiler_params=pltpu.CompilerParams(
            collective_id=0, has_side_effects=True, vmem_limit_bytes=MOVE_BYTES
        ),
    )(routes, gate_weight, up_weight)


def store_kernel(depth, piece, got_ref, scales_ref, gate_ref, up_ref, out_ref, sems):
    copies = [pltpu.make_async_copy(scales_ref, out_ref, sems.at[2 * got_ref.shape[0]])]
    for c in range(got_ref.shape[0]):
        for p, ref in enumerate((gate_ref, up_ref)):
            copies.append(
                pltpu.make_async_copy(
                    got_ref.at[c, pl.ds(p * depth, depth)],
                    ref.at[:, pl.ds(c * piece, piece)],
                    sems.at[2 * c + p],
                )
            )
    for copy in copies:
        copy.start()
    for copy in copies:
        copy.wait()


def store_call(got, scales):
    n_col, double, piece = got.shape
    depth = double // 2
    any_spec = pl.BlockSpec(memory_space=pl.ANY)
    return pl.pallas_call(
        functools.partial(store_kernel, depth, piece),
        in_specs=[pl.BlockSpec(memory_space=pltpu.VMEM), pl.BlockSpec(memory_space=pltpu.VMEM)],
        out_specs=[any_spec] * 3,
        out_shape=[
            jax.ShapeDtypeStruct((depth, n_col * piece), got.dtype),
            jax.ShapeDtypeStruct((depth, n_col * piece), got.dtype),
            jax.ShapeDtypeStruct((2, n_col * piece), jnp.float32),
        ],
        scratch_shapes=[pltpu.SemaphoreType.DMA((2 * n_col + 1,))],
        compiler_params=pltpu.CompilerParams(vmem_limit_bytes=STORE_BYTES),
    )(got, scales)


def kernel_shards(n_row, n_col, gate_weight, up_weight, routes):
    got, scales = move_call(gate_weight, up_weight, routes, n_row, n_col, PARTS)
    return tuple(store_call(got, scales))


def fits(n_row, n_col, height, width):
    if n_col % n_row or width % n_row or (width // n_row) % 128:
        return False
    ratio = n_col // n_row
    if height % (ratio * PARTS * 16) or height // (ratio * PARTS) < 48:
        return False
    held_bytes = ((2 * n_row - 1) * 2 * height + n_col * 2 * height // ratio) * (width // n_row) * 2
    return held_bytes < 60 * 1024 * 1024


def solution(mesh):
    n_row, n_col = mesh.shape["row"], mesh.shape["col"]

    def shards(gate_weight, up_weight, routes):
        if fits(n_row, n_col, *gate_weight.shape):
            return kernel_shards(n_row, n_col, gate_weight, up_weight, routes)
        return plain_shards(gate_weight, up_weight, routes)

    return jax.shard_map(
        shards,
        mesh=mesh,
        in_specs=(P("row", "col"), P("row", "col"), P()),
        out_specs=(P("col", "row"), P("col", "row"), P(None, "row")),
        check_vma=False,
    )
```

```python
import functools

import jax
import jax.numpy as jnp
from jax import lax
from jax.experimental import pallas as pl
from jax.experimental.pallas import tpu as pltpu
from jax.sharding import PartitionSpec as P

EPSILON = 1e-06
LIMIT = 4.0
MESH = pl.DeviceIdType.MESH
MOVE_BYTES = 40 * 1024 * 1024
STORE_BYTES = 1024 * 1024
RAW = 64
SMALL = 4
LARGE = 4
LAG = 2


def column_peaks(weight):
    return jnp.max(jnp.abs(weight), axis=0).astype(jnp.float32)


def quantize(weight, peaks):
    factor = LIMIT / (peaks + EPSILON)
    return (weight.astype(jnp.float32) * factor[None, :]).astype(jnp.bfloat16)


def order_pieces(weight, order, pieces):
    height, width = weight.shape
    shaped = weight.reshape(height, pieces, width // pieces)
    return jnp.take(shaped, order, axis=1).reshape(height, width)


def own_piece(peaks, pick, pieces):
    shaped = ((peaks + EPSILON) / LIMIT).reshape(pieces, -1)
    return lax.dynamic_index_in_dim(shaped, pick, 0, keepdims=False)


def exchange(sent):
    sent = lax.all_to_all(sent, "row", split_axis=1, concat_axis=0, tiled=True)
    return lax.all_to_all(sent, "col", split_axis=0, concat_axis=1, tiled=True)


def plain_shards(gate_weight, up_weight, routes):
    pieces = lax.axis_size("row")
    row_index = lax.axis_index("row")
    gate_peaks, up_peaks = lax.pmax((column_peaks(gate_weight), column_peaks(up_weight)), "row")
    gate_serving = exchange(order_pieces(quantize(gate_weight, gate_peaks), routes[0], pieces))
    up_serving = exchange(order_pieces(quantize(up_weight, up_peaks), routes[1], pieces))
    chosen = jnp.take(routes, row_index, axis=1)
    local_scales = jnp.stack(
        [own_piece(gate_peaks, chosen[0], pieces), own_piece(up_peaks, chosen[1], pieces)]
    )
    scales = lax.all_gather(local_scales, "col", axis=1, tiled=True)
    return (gate_serving, up_serving, scales)


def move_kernel(
    n_row, n_col, depth, raw, head, bodies,
    routes_ref, gate_ref, up_ref, got_ref, scales_ref,
    routes, sent, mid, tops, peak, peak_mid, total, factor, peak_all,
    route_load, load, send1, head1, body1, send2, recv2, peak_send, peak_recv,
):
    row, col = lax.axis_index("row"), lax.axis_index("col")
    ratio = n_col // n_row
    height = ratio * depth
    piece = sent.shape[2]
    heads = [(h, q, n) for q, n in head for h in range(ratio)]
    mine = row * ratio

    def peer_row(s):
        return lax.rem(row + s, n_row)

    def peer_col(s):
        return lax.rem(col + s, n_col)

    def local(ref, target, sem):
        return pltpu.make_async_copy(ref, target, sem)

    def wait_bytes(ref, sem):
        local(ref, ref, sem).wait()

    def remote(ref, target, send, recv, to_row, to_col):
        return pltpu.make_async_remote_copy(
            src_ref=ref, dst_ref=target, send_sem=send, recv_sem=recv,
            device_id=(to_row, to_col), device_id_type=MESH,
        )

    def fetch(p, h, start, n, index):
        ref = (gate_ref, up_ref)[p]
        for j in range(n_row):
            local(
                ref.at[pl.ds(h * depth + start, n), pl.ds(j * piece, piece)],
                sent.at[j, pl.ds(p * height + h * depth + start, n)],
                load.at[index],
            ).start()

    def fetched(p, h, start, n, index):
        wait_bytes(sent.at[:, pl.ds(p * height + h * depth + start, n)], load.at[index])

    def rows_of(h, p, start, n):
        src = pl.ds(pl.multiple_of((p * ratio + h) * depth + start, 16), n)
        dst = pl.ds(pl.multiple_of(p * depth + start, 16), n)
        return src, dst

    def start_first(sems, h, p, start, n):
        src, dst = rows_of(h, p, start, n)
        for s in range(1, n_row):
            to = peer_row(s)

            @pl.when(mine + h != col)
            def _():
                remote(sent.at[to, src], mid.at[n_row - 1 - s, src], send1, sems[s - 1], to, col).start()

            @pl.when(mine + h == col)
            def _():
                remote(sent.at[to, src], got_ref.at[col, dst], send1, sems[s - 1], to, col).start()

    def start_second(s, h, p, start, n, kind):
        src, dst = rows_of(h, p, start, n)
        to = peer_row(n_row - s) * ratio + h
        block = sent.at[row, src] if s == 0 else mid.at[n_row - 1 - s, src]

        @pl.when(to != col)
        def _():
            remote(block, got_ref.at[col, dst], send2, recv2.at[kind], row, to).start()

        if s == 0:
            @pl.when(to == col)
            def _():
                @pl.loop(0, n // 16)
                def _(g):
                    here = pl.ds(pl.multiple_of(src.start + g * 16, 16), 16)
                    there = pl.ds(pl.multiple_of(dst.start + g * 16, 16), 16)
                    got_ref[col, there, :] = sent[row, here, :]

    def pick(p, i, pieces):
        chosen = pieces[0]
        for j in range(1, n_row):
            chosen = jnp.where(routes[p, i] == j, pieces[j], chosen)
        return chosen

    def raise_tops(p, j, block):
        cols = pl.ds(j * piece, piece)
        best = tops[p, :, cols]
        for t in range(block.shape[0] // 16):
            best = jnp.maximum(best, jnp.abs(block[t * 16 : t * 16 + 16]))
        tops[p, :, cols] = best

    def prepare_head(h, start, n):
        @pl.loop(0, n // 16)
        def _(g):
            here = pl.ds(pl.multiple_of(h * depth + start + g * 16, 16), 16)
            pieces = [sent[j, here, :] for j in range(n_row)]
            for j in range(n_row):
                raise_tops(0, j, pieces[j])
            for i in range(n_row):
                sent[i, here, :] = pick(0, i, pieces)

    blocks = [(p, h) for p in range(2) for h in range(ratio)]

    def block_start(p):
        return raw if p == 0 else 0

    def scan_block(b):
        p, h = blocks[b]
        start = block_start(p)
        n = depth - start
        fetched(p, h, start, n, 2 * ratio + b)

        @pl.loop(0, n // 64)
        def _(g):
            here = pl.ds(pl.multiple_of(p * height + h * depth + start + g * 64, 16), 64)
            for j in range(n_row):
                raise_tops(p, j, sent[j, here, :])

    def head_sems(e):
        return [head1.at[e, s] for s in range(n_row - 1)]

    def begin_head(e):
        h, q, n = heads[e]
        start_first(head_sems(e), h, 0, q, n)
        start_second(0, h, 0, q, n, 0)

    def forward_head(e):
        h, q, n = heads[e]
        src, _ = rows_of(h, 0, q, n)
        for s in range(1, n_row):
            wait_bytes(mid.at[n_row - 1 - s, src], head1.at[e, s - 1])
            start_second(s, h, 0, q, n, 0)

    barrier = pltpu.get_barrier_semaphore()
    for s in sorted(range(1, n_col), key=lambda s: -min(s, n_col - s)):
        pl.semaphore_signal(barrier, inc=1, device_id=(row, peer_col(s)), device_id_type=MESH)
    for s in range(1, n_row):
        pl.semaphore_signal(barrier, inc=1, device_id=(peer_row(s), col), device_id_type=MESH)

    route_copy = local(routes_ref, routes, route_load)
    route_copy.start()
    first = head[0][1]
    for h in range(ratio):
        fetch(0, h, 0, first, h)
    for h in range(ratio):
        fetch(0, h, first, raw - first, ratio + h)
    for b, (p, h) in enumerate(blocks):
        start = block_start(p)
        fetch(p, h, start, depth - start, 2 * ratio + b)
    tops[...] = jnp.zeros_like(tops)

    route_copy.wait()
    for h in range(ratio):
        fetched(0, h, 0, first, h)
    for e in range(ratio):
        prepare_head(*heads[e])
    for h in range(ratio):
        fetched(0, h, first, raw - first, ratio + h)
    for e in range(ratio, len(heads)):
        prepare_head(*heads[e])
    scan_block(0)

    held = len(heads) - ratio
    pl.semaphore_wait(barrier, n_row + n_col - 2)
    for e in range(held):
        begin_head(e)
    scan_block(1)
    forward_head(0)
    scan_block(2)
    forward_head(1)
    for b in range(3, len(blocks)):
        scan_block(b)

    for p in range(2):
        pieces = [
            jnp.max(tops[p, :, pl.ds(j * piece, piece)].astype(jnp.float32), axis=0, keepdims=True)
            for j in range(n_row)
        ]
        for i in range(n_row):
            peak[i, pl.ds(p, 1), :] = pick(p, i, pieces)

    forward_head(2)
    for s in range(1, n_row):
        remote(peak, peak_mid.at[s - 1], peak_send.at[0], peak_recv.at[0], peer_row(s), col).start()
    for e in range(held, len(heads)):
        begin_head(e)
    for e in range(3, held):
        forward_head(e)

    wait_bytes(peak_mid, peak_recv.at[0])
    for i in range(n_row):
        top = peak[i]
        for s in range(1, n_row):
            top = jnp.maximum(top, peak_mid[s - 1, i])
        total[i] = top
        value = LIMIT / (top + EPSILON)
        for p in range(2):
            factor[p * n_row + i] = value[p : p + 1]

    late = list(range(held, len(heads)))
    base = 0
    for p, (start, size, count) in enumerate(bodies):
        def place(k, start=start, size=size):
            return lax.rem(k, ratio), start + (k // ratio) * size

        def prepare(k, p=p, size=size, place=place):
            h, at = place(k)
            src, _ = rows_of(h, p, at, size)

            @pl.loop(0, size // 16)
            def _(g):
                here = pl.ds(pl.multiple_of(src.start + g * 16, 16), 16)
                pieces = [sent[j, here, :] for j in range(n_row)]
                for i in range(n_row):
                    value = pick(p, i, pieces).astype(jnp.float32)
                    sent[i, here, :] = (value * factor[p * n_row + i]).astype(sent.dtype)

        def begin(k, p=p, size=size, base=base, place=place):
            h, at = place(k)
            start_first([body1.at[base + k]] * (n_row - 1), h, p, at, size)
            start_second(0, h, p, at, size, 1)

        def forward(k, p=p, size=size, base=base, place=place):
            h, at = place(k)
            src, _ = rows_of(h, p, at, size)
            wait_bytes(mid.at[:, src], body1.at[base + k])
            for s in range(1, n_row):
                start_second(s, h, p, at, size, 1)

        steps = count * ratio
        prepare(0)
        if p == 0:
            for s in range(1, n_col):
                remote(
                    total.at[row], peak_all.at[col], peak_send.at[1], peak_recv.at[1], row, peer_col(s)
                ).start()
            peak_all[col] = total[row]
        prepare(1)
        begin(0)
        for e in late:
            forward_head(e)
        late = []

        @pl.loop(1, steps + LAG)
        def _(k, steps=steps, prepare=prepare, begin=begin, forward=forward):
            @pl.when(k + 1 < steps)
            def _():
                prepare(k + 1)

            @pl.when(k < steps)
            def _():
                begin(k)

            @pl.when(k >= LAG)
            def _():
                forward(k - LAG)

        base += steps

    others = pl.ds(0, n_col - 1)
    wait_bytes(peak_all.at[others], peak_send.at[1])
    wait_bytes(peak_all.at[others], peak_recv.at[1])
    wait_bytes(got_ref.at[others, pl.ds(0, raw)], recv2.at[0])
    for c in range(n_col):
        base_peak = peak_all[c] + EPSILON
        scales_ref[:, pl.ds(c * piece, piece)] = base_peak / LIMIT
        value = (LIMIT / base_peak)[0:1]

        @pl.loop(0, raw // 16)
        def _(g):
            here = pl.ds(pl.multiple_of(g * 16, 16), 16)
            got_ref[c, here, :] = (got_ref[c, here, :].astype(jnp.float32) * value).astype(got_ref.dtype)

    wait_bytes(peak_mid, peak_send.at[0])
    wait_bytes(mid, send1)
    wait_bytes(got_ref.at[others], send2)
    wait_bytes(got_ref.at[others, pl.ds(raw, 2 * depth - raw)], recv2.at[1])


def move_call(gate_weight, up_weight, routes, n_row, n_col):
    height, width = gate_weight.shape
    kind = gate_weight.dtype
    piece = width // n_row
    ratio = n_col // n_row
    depth = height // ratio
    head = [(0, 16), (16, 16), (32, RAW - 32)]
    small = SMALL * 16
    large = depth // LARGE
    bodies = [(RAW, small, (depth - RAW) // small), (0, large, LARGE)]
    steps = sum(count for _, _, count in bodies) * ratio
    dma = pltpu.SemaphoreType.DMA
    return pl.pallas_call(
        functools.partial(move_kernel, n_row, n_col, depth, RAW, head, bodies),
        out_shape=[
            pltpu.VMEM((n_col, 2 * depth, piece), kind),
            pltpu.VMEM((2, n_col * piece), jnp.float32),
        ],
        in_specs=[pl.BlockSpec(memory_space=pl.ANY)] * 3,
        out_specs=[
            pl.BlockSpec(memory_space=pltpu.VMEM),
            pl.BlockSpec(memory_space=pltpu.VMEM),
        ],
        scratch_shapes=[
            pltpu.SMEM(routes.shape, routes.dtype),
            pltpu.VMEM((n_row, 2 * height, piece), kind),
            pltpu.VMEM((n_row - 1, 2 * height, piece), kind),
            pltpu.VMEM((2, 16, width), kind),
            pltpu.VMEM((n_row, 2, piece), jnp.float32),
            pltpu.VMEM((n_row - 1, n_row, 2, piece), jnp.float32),
            pltpu.VMEM((n_row, 2, piece), jnp.float32),
            pltpu.VMEM((2 * n_row, 1, piece), jnp.float32),
            pltpu.VMEM((n_col, 2, piece), jnp.float32),
            dma,
            dma((4 * ratio,)),
            dma,
            dma((len(head) * ratio, n_row - 1)),
            dma((steps,)),
            dma,
            dma((2,)),
            dma((2,)),
            dma((2,)),
        ],
        compiler_params=pltpu.CompilerParams(
            collective_id=0, has_side_effects=True, vmem_limit_bytes=MOVE_BYTES
        ),
    )(routes, gate_weight, up_weight)


def store_kernel(depth, piece, got_ref, scales_ref, gate_ref, up_ref, out_ref, sems):
    copies = [pltpu.make_async_copy(scales_ref, out_ref, sems.at[2 * got_ref.shape[0]])]
    for c in range(got_ref.shape[0]):
        for p, ref in enumerate((gate_ref, up_ref)):
            copies.append(
                pltpu.make_async_copy(
                    got_ref.at[c, pl.ds(p * depth, depth)],
                    ref.at[:, pl.ds(c * piece, piece)],
                    sems.at[2 * c + p],
                )
            )
    for copy in copies:
        copy.start()
    for copy in copies:
        copy.wait()


def store_call(got, scales):
    n_col, double, piece = got.shape
    depth = double // 2
    any_spec = pl.BlockSpec(memory_space=pl.ANY)
    return pl.pallas_call(
        functools.partial(store_kernel, depth, piece),
        in_specs=[pl.BlockSpec(memory_space=pltpu.VMEM), pl.BlockSpec(memory_space=pltpu.VMEM)],
        out_specs=[any_spec] * 3,
        out_shape=[
            jax.ShapeDtypeStruct((depth, n_col * piece), got.dtype),
            jax.ShapeDtypeStruct((depth, n_col * piece), got.dtype),
            jax.ShapeDtypeStruct((2, n_col * piece), jnp.float32),
        ],
        scratch_shapes=[pltpu.SemaphoreType.DMA((2 * n_col + 1,))],
        compiler_params=pltpu.CompilerParams(vmem_limit_bytes=STORE_BYTES),
    )(got, scales)


def kernel_shards(n_row, n_col, gate_weight, up_weight, routes):
    got, scales = move_call(gate_weight, up_weight, routes, n_row, n_col)
    return tuple(store_call(got, scales))


def fits(n_row, n_col, height, width):
    if n_col % n_row or width % n_row or (width // n_row) % 128:
        return False
    ratio = n_col // n_row
    depth = height // ratio
    if ratio != 2 or height % ratio or depth % (LARGE * 16) or depth % 64 or (depth - RAW) % (SMALL * 16):
        return False
    held_bytes = ((2 * n_row - 1) * 2 * height + n_col * 2 * height // ratio) * (width // n_row) * 2
    return held_bytes < 60 * 1024 * 1024


def solution(mesh):
    n_row, n_col = mesh.shape["row"], mesh.shape["col"]

    def shards(gate_weight, up_weight, routes):
        if fits(n_row, n_col, *gate_weight.shape):
            return kernel_shards(n_row, n_col, gate_weight, up_weight, routes)
        return plain_shards(gate_weight, up_weight, routes)

    return jax.shard_map(
        shards,
        mesh=mesh,
        in_specs=(P("row", "col"), P("row", "col"), P()),
        out_specs=(P("col", "row"), P("col", "row"), P(None, "row")),
        check_vma=False,
    )
```

```python
import functools

import jax
import jax.numpy as jnp
from jax import lax
from jax.experimental import pallas as pl
from jax.experimental.pallas import tpu as pltpu
from jax.sharding import PartitionSpec as P

EPSILON = 1e-06
LIMIT = 4.0
MESH = pl.DeviceIdType.MESH
MOVE_BYTES = 40 * 1024 * 1024
STORE_BYTES = 1024 * 1024
RAW = 64
SMALL = 4
LARGE = 5
MINI = 16
LAG = 2


def column_peaks(weight):
    return jnp.max(jnp.abs(weight), axis=0).astype(jnp.float32)


def quantize(weight, peaks):
    factor = LIMIT / (peaks + EPSILON)
    return (weight.astype(jnp.float32) * factor[None, :]).astype(jnp.bfloat16)


def order_pieces(weight, order, pieces):
    height, width = weight.shape
    shaped = weight.reshape(height, pieces, width // pieces)
    return jnp.take(shaped, order, axis=1).reshape(height, width)


def own_piece(peaks, pick, pieces):
    shaped = ((peaks + EPSILON) / LIMIT).reshape(pieces, -1)
    return lax.dynamic_index_in_dim(shaped, pick, 0, keepdims=False)


def exchange(sent):
    sent = lax.all_to_all(sent, "row", split_axis=1, concat_axis=0, tiled=True)
    return lax.all_to_all(sent, "col", split_axis=0, concat_axis=1, tiled=True)


def plain_shards(gate_weight, up_weight, routes):
    pieces = lax.axis_size("row")
    row_index = lax.axis_index("row")
    gate_peaks, up_peaks = lax.pmax((column_peaks(gate_weight), column_peaks(up_weight)), "row")
    gate_serving = exchange(order_pieces(quantize(gate_weight, gate_peaks), routes[0], pieces))
    up_serving = exchange(order_pieces(quantize(up_weight, up_peaks), routes[1], pieces))
    chosen = jnp.take(routes, row_index, axis=1)
    local_scales = jnp.stack(
        [own_piece(gate_peaks, chosen[0], pieces), own_piece(up_peaks, chosen[1], pieces)]
    )
    scales = lax.all_gather(local_scales, "col", axis=1, tiled=True)
    return (gate_serving, up_serving, scales)


def move_kernel(
    n_row, n_col, depth, raw, head, mini, bodies,
    routes_ref, gate_ref, up_ref, got_ref, scales_ref,
    routes, sent, mid, relay, tops, peak, peak_mid, total, factor, peak_all,
    route_load, load, send1, head1, mini1, body1, send2, recv2, peak_send, peak_recv, relay_sems,
):
    row, col = lax.axis_index("row"), lax.axis_index("col")
    ratio = n_col // n_row
    height = ratio * depth
    piece = sent.shape[2]
    heads = [(h, q, n) for q, n in head for h in range(ratio)]
    mine = row * ratio

    half = n_row // 2
    near = [half] + [half + t * (1 - 2 * (row % 2)) for u in range(1, half) for t in (u, -u)]
    close = [half] + [half - t * (1 - 2 * (row % 2)) for u in range(1, half) for t in (u, -u)]
    far = [s + (row // half) * (n_row - 2 * s) for s in range(1, n_row)]

    def peer_row(s):
        return lax.rem(row + s, n_row)

    def peer_col(s):
        return lax.rem(col + s, n_col)

    def local(ref, target, sem):
        return pltpu.make_async_copy(ref, target, sem)

    def wait_bytes(ref, sem):
        local(ref, ref, sem).wait()

    def remote(ref, target, send, recv, to_row, to_col):
        return pltpu.make_async_remote_copy(
            src_ref=ref, dst_ref=target, send_sem=send, recv_sem=recv,
            device_id=(to_row, to_col), device_id_type=MESH,
        )

    def fetch(p, h, start, n, index):
        ref = (gate_ref, up_ref)[p]
        for j in range(n_row):
            local(
                ref.at[pl.ds(h * depth + start, n), pl.ds(j * piece, piece)],
                sent.at[j, pl.ds(p * height + h * depth + start, n)],
                load.at[index],
            ).start()

    def fetched(p, h, start, n, index):
        wait_bytes(sent.at[:, pl.ds(p * height + h * depth + start, n)], load.at[index])

    def rows_of(h, p, start, n):
        src = pl.ds(pl.multiple_of((p * ratio + h) * depth + start, 16), n)
        dst = pl.ds(pl.multiple_of(p * depth + start, 16), n)
        return src, dst

    def start_first(sems, h, p, start, n):
        src, dst = rows_of(h, p, start, n)
        for s in near:
            to = peer_row(s)

            @pl.when(mine + h != col)
            def _():
                remote(sent.at[to, src], mid.at[n_row - 1 - s, src], send1, sems(s), to, col).start()

            @pl.when(mine + h == col)
            def _():
                remote(sent.at[to, src], got_ref.at[col, dst], send1, sems(s), to, col).start()

    def start_second(s, h, p, start, n, kind, send=0):
        src, dst = rows_of(h, p, start, n)
        to = peer_row(n_row - s) * ratio + h
        own = isinstance(s, int) and s == 0
        block = sent.at[row, src] if own else mid.at[n_row - 1 - s, src]

        @pl.when(to != col)
        def _():
            remote(block, got_ref.at[col, dst], send2.at[send], recv2.at[kind], row, to).start()

        if own:
            @pl.when(to == col)
            def _():
                @pl.loop(0, n // 16)
                def _(g):
                    here = pl.ds(pl.multiple_of(src.start + g * 16, 16), 16)
                    there = pl.ds(pl.multiple_of(dst.start + g * 16, 16), 16)
                    got_ref[col, there, :] = sent[row, here, :]

    def pick(p, i, pieces):
        chosen = pieces[0]
        for j in range(1, n_row):
            chosen = jnp.where(routes[p, i] == j, pieces[j], chosen)
        return chosen

    def raise_tops(p, j, block):
        cols = pl.ds(j * piece, piece)
        best = tops[p, :, cols]
        for t in range(block.shape[0] // 16):
            best = jnp.maximum(best, jnp.abs(block[t * 16 : t * 16 + 16]))
        tops[p, :, cols] = best

    def prepare_head(h, start, n):
        @pl.loop(0, n // 16)
        def _(g):
            here = pl.ds(pl.multiple_of(h * depth + start + g * 16, 16), 16)
            pieces = [sent[j, here, :] for j in range(n_row)]
            for j in range(n_row):
                raise_tops(0, j, pieces[j])
            for i in range(n_row):
                sent[i, here, :] = pick(0, i, pieces)

    blocks = [(p, h) for p in range(2) for h in range(ratio)]

    def block_start(p):
        return raw if p == 0 else 0

    def scan_block(b):
        p, h = blocks[b]
        start = block_start(p)
        n = depth - start
        fetched(p, h, start, n, 2 * ratio + b)

        @pl.loop(0, n // 64)
        def _(g):
            here = pl.ds(pl.multiple_of(p * height + h * depth + start + g * 64, 16), 64)
            for j in range(n_row):
                raise_tops(p, j, sent[j, here, :])

    def head_sems(e):
        return lambda s: head1.at[e, s - 1]

    def begin_head(e):
        h, q, n = heads[e]
        start_first(head_sems(e), h, 0, q, n)
        start_second(0, h, 0, q, n, 0)

    def forward_head(e):
        h, q, n = heads[e]
        src, _ = rows_of(h, 0, q, n)
        for s in close:
            wait_bytes(mid.at[n_row - 1 - s, src], head1.at[e, s - 1])
            start_second(s, h, 0, q, n, 0)

    barrier = pltpu.get_barrier_semaphore()
    for s in sorted(range(1, n_col), key=lambda s: -min(s, n_col - s)):
        pl.semaphore_signal(barrier, inc=1, device_id=(row, peer_col(s)), device_id_type=MESH)
    for s in range(1, n_row):
        pl.semaphore_signal(barrier, inc=1, device_id=(peer_row(s), col), device_id_type=MESH)

    route_copy = local(routes_ref, routes, route_load)
    route_copy.start()
    first = head[0][1]
    for h in range(ratio):
        fetch(0, h, 0, first, h)
    for h in range(ratio):
        fetch(0, h, first, raw - first, ratio + h)
    for b, (p, h) in enumerate(blocks):
        start = block_start(p)
        fetch(p, h, start, depth - start, 2 * ratio + b)
    tops[...] = jnp.zeros_like(tops)

    route_copy.wait()
    for h in range(ratio):
        fetched(0, h, 0, first, h)
    for e in range(ratio):
        prepare_head(*heads[e])
    for h in range(ratio):
        fetched(0, h, first, raw - first, ratio + h)
    for e in range(ratio, len(heads)):
        prepare_head(*heads[e])
    held = len(heads) - ratio
    pl.semaphore_wait(barrier, n_row + n_col - 2)
    for e in range(held):
        begin_head(e)
    scan_block(0)
    forward_head(0)
    forward_head(1)
    scan_block(1)
    scan_block(2)
    for b in range(3, len(blocks)):
        scan_block(b)

    for p in range(2):
        pieces = [
            jnp.max(tops[p, :, pl.ds(j * piece, piece)].astype(jnp.float32), axis=0, keepdims=True)
            for j in range(n_row)
        ]
        for i in range(n_row):
            peak[i, pl.ds(p, 1), :] = pick(p, i, pieces)

    forward_head(2)
    for s in range(1, n_row):
        remote(peak, peak_mid.at[s - 1], peak_send.at[0], peak_recv.at[0], peer_row(s), col).start()
    for e in range(held, len(heads)):
        begin_head(e)
    for e in range(3, held):
        forward_head(e)

    wait_bytes(peak_mid, peak_recv.at[0])
    for i in range(n_row):
        top = peak[i]
        for s in range(1, n_row):
            top = jnp.maximum(top, peak_mid[s - 1, i])
        total[i] = top
        value = LIMIT / (top + EPSILON)
        for p in range(2):
            factor[p * n_row + i] = value[p : p + 1]

    def prepare_rows(h, p, start, n):
        src, _ = rows_of(h, p, start, n)

        @pl.loop(0, n // 16)
        def _(g):
            here = pl.ds(pl.multiple_of(src.start + g * 16, 16), 16)
            pieces = [sent[j, here, :] for j in range(n_row)]
            for i in range(n_row):
                value = pick(p, i, pieces).astype(jnp.float32)
                sent[i, here, :] = (value * factor[p * n_row + i]).astype(sent.dtype)

    back = peer_row(n_row - half) * ratio

    def begin_mini(h):
        src, dst = rows_of(h, 1, 0, mini)
        for t, s in enumerate(near):
            to = peer_row(s)

            @pl.when(mine + h == col)
            def _():
                remote(sent.at[to, src], got_ref.at[col, dst], send1, mini1.at[h, s - 1], to, col).start()

            @pl.when(mine + h != col)
            def _():
                if h == 0 and t == 0:
                    remote(sent.at[to, src], relay.at[col], send1, relay_sems.at[0], row, mine).start()
                else:
                    remote(sent.at[to, src], mid.at[n_row - 1 - s, src], send1, mini1.at[h, s - 1], to, col).start()
        start_second(0, h, 1, 0, mini, 1, 1)

    def forward_mini(h):
        src, _ = rows_of(h, 1, 0, mini)
        for t, s in enumerate(close):
            block = mid.at[n_row - 1 - s, src]
            if h == 0 and t == 0:
                @pl.when(back == col)
                def _():
                    wait_bytes(block, mini1.at[h, s - 1])
            else:
                wait_bytes(block, mini1.at[h, s - 1])
                start_second(s, h, 1, 0, mini, 1, 1)

    late = list(range(held, len(heads)))
    base = 0
    for p, (start, size, count) in enumerate(bodies):
        def place(k, start=start, size=size):
            return lax.rem(k, ratio), start + (k // ratio) * size

        def prepare(k, p=p, size=size, place=place):
            h, at = place(k)
            prepare_rows(h, p, at, size)

        def begin(k, p=p, size=size, base=base, place=place):
            h, at = place(k)
            start_first(lambda s: body1.at[base + k], h, p, at, size)
            start_second(0, h, p, at, size, 1)

        def forward(k, p=p, size=size, base=base, place=place):
            h, at = place(k)
            src, _ = rows_of(h, p, at, size)
            wait_bytes(mid.at[:, src], body1.at[base + k])
            for s in far:
                start_second(s, h, p, at, size, 1)

        steps = count * ratio
        if p == 0:
            for h in range(ratio):
                prepare_rows(h, 1, 0, mini)
        prepare(0)
        if p == 0:
            for h in range(ratio):
                begin_mini(h)
            for s in range(1, n_col):
                remote(
                    total.at[row], peak_all.at[col], peak_send.at[1], peak_recv.at[1], row, peer_col(s)
                ).start()
            peak_all[col] = total[row]
        prepare(1)
        begin(0)
        for e in late:
            forward_head(e)
        if p == 0:
            for h in range(ratio):
                forward_mini(h)
        late = []

        @pl.loop(1, steps + LAG)
        def _(k, steps=steps, prepare=prepare, begin=begin, forward=forward):
            @pl.when(k + 1 < steps)
            def _():
                prepare(k + 1)

            @pl.when(k < steps)
            def _():
                begin(k)

            @pl.when(k >= LAG)
            def _():
                forward(k - LAG)

        base += steps

    others = pl.ds(0, n_col - 1)

    @pl.when(mine == col)
    def _():
        wait_bytes(relay.at[others], relay_sems.at[0])
        _, dst = rows_of(0, 1, 0, mini)
        for s in range(1, n_col):
            other = peer_col(s)
            remote(
                relay.at[other], got_ref.at[other, dst], relay_sems.at[1], recv2.at[1], peer_row(half), col
            ).start()

    wait_bytes(peak_all.at[others], peak_send.at[1])
    wait_bytes(peak_all.at[others], peak_recv.at[1])
    wait_bytes(got_ref.at[others, pl.ds(0, raw)], recv2.at[0])
    for c in range(n_col):
        base_peak = peak_all[c] + EPSILON
        scales_ref[:, pl.ds(c * piece, piece)] = base_peak / LIMIT
        value = (LIMIT / base_peak)[0:1]

        @pl.loop(0, raw // 16)
        def _(g):
            here = pl.ds(pl.multiple_of(g * 16, 16), 16)
            got_ref[c, here, :] = (got_ref[c, here, :].astype(jnp.float32) * value).astype(got_ref.dtype)

    wait_bytes(peak_mid, peak_send.at[0])
    wait_bytes(mid, send1)
    wait_bytes(got_ref.at[others, pl.ds(0, 2 * depth - mini)], send2.at[0])

    @pl.when(back == col)
    def _():
        wait_bytes(sent.at[0, pl.ds(0, (n_row * ratio - 1) * mini)], send2.at[1])

    @pl.when(back != col)
    def _():
        wait_bytes(sent.at[0, pl.ds(0, (n_row * ratio - 2) * mini)], send2.at[1])

    @pl.when(mine == col)
    def _():
        wait_bytes(relay.at[others], relay_sems.at[1])

    wait_bytes(got_ref.at[others, pl.ds(raw, 2 * depth - raw)], recv2.at[1])


def move_call(gate_weight, up_weight, routes, n_row, n_col):
    height, width = gate_weight.shape
    kind = gate_weight.dtype
    piece = width // n_row
    ratio = n_col // n_row
    depth = height // ratio
    head = [(q, 16) for q in range(0, RAW, 16)]
    small = SMALL * 16
    large = (depth - MINI) // LARGE
    bodies = [(RAW, small, (depth - RAW) // small), (MINI, large, LARGE)]
    steps = sum(count for _, _, count in bodies) * ratio
    dma = pltpu.SemaphoreType.DMA
    return pl.pallas_call(
        functools.partial(move_kernel, n_row, n_col, depth, RAW, head, MINI, bodies),
        out_shape=[
            pltpu.VMEM((n_col, 2 * depth, piece), kind),
            pltpu.VMEM((2, n_col * piece), jnp.float32),
        ],
        in_specs=[pl.BlockSpec(memory_space=pl.ANY)] * 3,
        out_specs=[
            pl.BlockSpec(memory_space=pltpu.VMEM),
            pl.BlockSpec(memory_space=pltpu.VMEM),
        ],
        scratch_shapes=[
            pltpu.SMEM(routes.shape, routes.dtype),
            pltpu.VMEM((n_row, 2 * height, piece), kind),
            pltpu.VMEM((n_row - 1, 2 * height, piece), kind),
            pltpu.VMEM((n_col, MINI, piece), kind),
            pltpu.VMEM((2, 16, width), kind),
            pltpu.VMEM((n_row, 2, piece), jnp.float32),
            pltpu.VMEM((n_row - 1, n_row, 2, piece), jnp.float32),
            pltpu.VMEM((n_row, 2, piece), jnp.float32),
            pltpu.VMEM((2 * n_row, 1, piece), jnp.float32),
            pltpu.VMEM((n_col, 2, piece), jnp.float32),
            dma,
            dma((4 * ratio,)),
            dma,
            dma((len(head) * ratio, n_row - 1)),
            dma((ratio, n_row - 1)),
            dma((steps,)),
            dma((2,)),
            dma((2,)),
            dma((2,)),
            dma((2,)),
            dma((2,)),
        ],
        compiler_params=pltpu.CompilerParams(
            collective_id=0, has_side_effects=True, vmem_limit_bytes=MOVE_BYTES
        ),
    )(routes, gate_weight, up_weight)


def store_kernel(depth, piece, got_ref, scales_ref, gate_ref, up_ref, out_ref, sems):
    for c in range(got_ref.shape[0]):
        for p, ref in enumerate((gate_ref, up_ref)):
            block = got_ref.at[c, pl.ds(p * depth, depth)]
            pltpu.make_async_copy(block, ref.at[:, pl.ds(c * piece, piece)], sems.at[0]).start()
    scales = pltpu.make_async_copy(scales_ref, out_ref, sems.at[1])
    scales.start()
    pltpu.make_async_copy(got_ref, got_ref, sems.at[0]).wait()
    scales.wait()


def store_call(got, scales):
    n_col, double, piece = got.shape
    depth = double // 2
    any_spec = pl.BlockSpec(memory_space=pl.ANY)
    return pl.pallas_call(
        functools.partial(store_kernel, depth, piece),
        in_specs=[pl.BlockSpec(memory_space=pltpu.VMEM), pl.BlockSpec(memory_space=pltpu.VMEM)],
        out_specs=[any_spec] * 3,
        out_shape=[
            jax.ShapeDtypeStruct((depth, n_col * piece), got.dtype),
            jax.ShapeDtypeStruct((depth, n_col * piece), got.dtype),
            jax.ShapeDtypeStruct((2, n_col * piece), jnp.float32),
        ],
        scratch_shapes=[pltpu.SemaphoreType.DMA((2,))],
        compiler_params=pltpu.CompilerParams(vmem_limit_bytes=STORE_BYTES),
    )(got, scales)


def kernel_shards(n_row, n_col, gate_weight, up_weight, routes):
    got, scales = move_call(gate_weight, up_weight, routes, n_row, n_col)
    return tuple(store_call(got, scales))


def fits(n_row, n_col, height, width):
    if n_col % n_row or width % n_row or (width // n_row) % 128:
        return False
    ratio = n_col // n_row
    depth = height // ratio
    if ratio != 2 or n_row != 4 or height % ratio or (depth - MINI) % (LARGE * 16) or depth % 64 or (depth - RAW) % (SMALL * 16):
        return False
    held_bytes = ((2 * n_row - 1) * 2 * height + n_col * 2 * height // ratio) * (width // n_row) * 2
    return held_bytes < 60 * 1024 * 1024


def solution(mesh):
    n_row, n_col = mesh.shape["row"], mesh.shape["col"]

    def shards(gate_weight, up_weight, routes):
        if fits(n_row, n_col, *gate_weight.shape):
            return kernel_shards(n_row, n_col, gate_weight, up_weight, routes)
        return plain_shards(gate_weight, up_weight, routes)

    return jax.shard_map(
        shards,
        mesh=mesh,
        in_specs=(P("row", "col"), P("row", "col"), P()),
        out_specs=(P("col", "row"), P("col", "row"), P(None, "row")),
        check_vma=False,
    )
```

```python
import functools

import jax
import jax.numpy as jnp
from jax import lax
from jax.experimental import pallas as pl
from jax.experimental.pallas import tpu as pltpu
from jax.sharding import PartitionSpec as P

EPSILON = 1e-06
LIMIT = 4.0
MESH = pl.DeviceIdType.MESH
MOVE_BYTES = 40 * 1024 * 1024
STORE_BYTES = 1024 * 1024
RAW = 64
SMALL = 8
LARGE = 5
MINI = 16
LAG = 2


def column_peaks(weight):
    return jnp.max(jnp.abs(weight), axis=0).astype(jnp.float32)


def quantize(weight, peaks):
    factor = LIMIT / (peaks + EPSILON)
    return (weight.astype(jnp.float32) * factor[None, :]).astype(jnp.bfloat16)


def order_pieces(weight, order, pieces):
    height, width = weight.shape
    shaped = weight.reshape(height, pieces, width // pieces)
    return jnp.take(shaped, order, axis=1).reshape(height, width)


def own_piece(peaks, pick, pieces):
    shaped = ((peaks + EPSILON) / LIMIT).reshape(pieces, -1)
    return lax.dynamic_index_in_dim(shaped, pick, 0, keepdims=False)


def exchange(sent):
    sent = lax.all_to_all(sent, "row", split_axis=1, concat_axis=0, tiled=True)
    return lax.all_to_all(sent, "col", split_axis=0, concat_axis=1, tiled=True)


def plain_shards(gate_weight, up_weight, routes):
    pieces = lax.axis_size("row")
    row_index = lax.axis_index("row")
    gate_peaks, up_peaks = lax.pmax((column_peaks(gate_weight), column_peaks(up_weight)), "row")
    gate_serving = exchange(order_pieces(quantize(gate_weight, gate_peaks), routes[0], pieces))
    up_serving = exchange(order_pieces(quantize(up_weight, up_peaks), routes[1], pieces))
    chosen = jnp.take(routes, row_index, axis=1)
    local_scales = jnp.stack(
        [own_piece(gate_peaks, chosen[0], pieces), own_piece(up_peaks, chosen[1], pieces)]
    )
    scales = lax.all_gather(local_scales, "col", axis=1, tiled=True)
    return (gate_serving, up_serving, scales)


def move_kernel(
    n_row, n_col, depth, raw, head, mini, bodies,
    routes_ref, gate_ref, up_ref, got_ref, scales_ref,
    routes, sent, mid, relay, tops, peak, peak_mid, total, factor, peak_all,
    route_load, load, send1, head1, mini1, body1, send2, recv2, peak_send, peak_recv, relay_sems,
):
    row, col = lax.axis_index("row"), lax.axis_index("col")
    ratio = n_col // n_row
    height = ratio * depth
    piece = sent.shape[2]
    heads = [(h, q, n) for q, n in head for h in range(ratio)]
    mine = row * ratio

    half = n_row // 2
    near = [half] + [half + t * (1 - 2 * (row % 2)) for u in range(1, half) for t in (u, -u)]
    close = [half] + [half - t * (1 - 2 * (row % 2)) for u in range(1, half) for t in (u, -u)]
    far = [s + (row // half) * (n_row - 2 * s) for s in range(1, n_row)]

    def peer_row(s):
        return lax.rem(row + s, n_row)

    def peer_col(s):
        return lax.rem(col + s, n_col)

    def local(ref, target, sem):
        return pltpu.make_async_copy(ref, target, sem)

    def wait_bytes(ref, sem):
        local(ref, ref, sem).wait()

    def remote(ref, target, send, recv, to_row, to_col):
        return pltpu.make_async_remote_copy(
            src_ref=ref, dst_ref=target, send_sem=send, recv_sem=recv,
            device_id=(to_row, to_col), device_id_type=MESH,
        )

    def fetch(p, h, start, n, index):
        ref = (gate_ref, up_ref)[p]
        for j in range(n_row):
            local(
                ref.at[pl.ds(h * depth + start, n), pl.ds(j * piece, piece)],
                sent.at[j, pl.ds(p * height + h * depth + start, n)],
                load.at[index],
            ).start()

    def fetched(p, h, start, n, index):
        wait_bytes(sent.at[:, pl.ds(p * height + h * depth + start, n)], load.at[index])

    def rows_of(h, p, start, n):
        src = pl.ds(pl.multiple_of((p * ratio + h) * depth + start, 16), n)
        dst = pl.ds(pl.multiple_of(p * depth + start, 16), n)
        return src, dst

    def start_first(sems, h, p, start, n):
        src, dst = rows_of(h, p, start, n)
        for s in near:
            to = peer_row(s)

            @pl.when(mine + h != col)
            def _():
                remote(sent.at[to, src], mid.at[n_row - 1 - s, src], send1, sems(s), to, col).start()

            @pl.when(mine + h == col)
            def _():
                remote(sent.at[to, src], got_ref.at[col, dst], send1, sems(s), to, col).start()

    def start_second(s, h, p, start, n, kind, send=0):
        src, dst = rows_of(h, p, start, n)
        to = peer_row(n_row - s) * ratio + h
        own = isinstance(s, int) and s == 0
        block = sent.at[row, src] if own else mid.at[n_row - 1 - s, src]

        @pl.when(to != col)
        def _():
            remote(block, got_ref.at[col, dst], send2.at[send], recv2.at[kind], row, to).start()

        if own:
            @pl.when(to == col)
            def _():
                @pl.loop(0, n // 16)
                def _(g):
                    here = pl.ds(pl.multiple_of(src.start + g * 16, 16), 16)
                    there = pl.ds(pl.multiple_of(dst.start + g * 16, 16), 16)
                    got_ref[col, there, :] = sent[row, here, :]

    def pick(p, i, pieces):
        chosen = pieces[0]
        for j in range(1, n_row):
            chosen = jnp.where(routes[p, i] == j, pieces[j], chosen)
        return chosen

    def raise_tops(p, j, block):
        cols = pl.ds(j * piece, piece)
        best = tops[p, :, cols]
        for t in range(block.shape[0] // 16):
            best = jnp.maximum(best, jnp.abs(block[t * 16 : t * 16 + 16]))
        tops[p, :, cols] = best

    def prepare_head(h, start, n):
        @pl.loop(0, n // 16)
        def _(g):
            here = pl.ds(pl.multiple_of(h * depth + start + g * 16, 16), 16)
            pieces = [sent[j, here, :] for j in range(n_row)]
            for j in range(n_row):
                raise_tops(0, j, pieces[j])
            for i in range(n_row):
                sent[i, here, :] = pick(0, i, pieces)

    blocks = [(p, h) for p in range(2) for h in range(ratio)]

    def block_start(p):
        return raw if p == 0 else 0

    def scan_block(b):
        p, h = blocks[b]
        start = block_start(p)
        n = depth - start
        fetched(p, h, start, n, 2 * ratio + b)

        @pl.loop(0, n // 64)
        def _(g):
            here = pl.ds(pl.multiple_of(p * height + h * depth + start + g * 64, 16), 64)
            for j in range(n_row):
                raise_tops(p, j, sent[j, here, :])

    def head_sems(e):
        return lambda s: head1.at[e, s - 1]

    def begin_head(e):
        h, q, n = heads[e]
        start_first(head_sems(e), h, 0, q, n)
        start_second(0, h, 0, q, n, 0)

    def forward_head(e):
        h, q, n = heads[e]
        src, _ = rows_of(h, 0, q, n)
        for s in close:
            wait_bytes(mid.at[n_row - 1 - s, src], head1.at[e, s - 1])
            start_second(s, h, 0, q, n, 0)

    barrier = pltpu.get_barrier_semaphore()
    for s in sorted(range(1, n_col), key=lambda s: -min(s, n_col - s)):
        pl.semaphore_signal(barrier, inc=1, device_id=(row, peer_col(s)), device_id_type=MESH)
    for s in range(1, n_row):
        pl.semaphore_signal(barrier, inc=1, device_id=(peer_row(s), col), device_id_type=MESH)

    route_copy = local(routes_ref, routes, route_load)
    route_copy.start()
    first = head[0][1]
    for h in range(ratio):
        fetch(0, h, 0, first, h)
    for h in range(ratio):
        fetch(0, h, first, raw - first, ratio + h)
    for b, (p, h) in enumerate(blocks):
        start = block_start(p)
        fetch(p, h, start, depth - start, 2 * ratio + b)
    tops[...] = jnp.zeros_like(tops)

    route_copy.wait()
    for h in range(ratio):
        fetched(0, h, 0, first, h)
    for e in range(ratio):
        prepare_head(*heads[e])
    for h in range(ratio):
        fetched(0, h, first, raw - first, ratio + h)
    for e in range(ratio, len(heads)):
        prepare_head(*heads[e])
    held = len(heads) - 2 * ratio
    pl.semaphore_wait(barrier, n_row + n_col - 2)
    for e in range(held):
        begin_head(e)
    scan_block(0)
    forward_head(0)
    forward_head(1)
    scan_block(1)
    scan_block(2)
    for b in range(3, len(blocks)):
        scan_block(b)

    for p in range(2):
        pieces = [
            jnp.max(tops[p, :, pl.ds(j * piece, piece)].astype(jnp.float32), axis=0, keepdims=True)
            for j in range(n_row)
        ]
        for i in range(n_row):
            peak[i, pl.ds(p, 1), :] = pick(p, i, pieces)

    forward_head(2)
    for s in range(1, n_row):
        remote(peak, peak_mid.at[s - 1], peak_send.at[0], peak_recv.at[0], peer_row(s), col).start()
    for e in range(held, len(heads)):
        begin_head(e)
    for e in range(3, held):
        forward_head(e)

    wait_bytes(peak_mid, peak_recv.at[0])
    for i in range(n_row):
        top = peak[i]
        for s in range(1, n_row):
            top = jnp.maximum(top, peak_mid[s - 1, i])
        total[i] = top
        value = LIMIT / (top + EPSILON)
        for p in range(2):
            factor[p * n_row + i] = value[p : p + 1]

    def prepare_rows(h, p, start, n):
        src, _ = rows_of(h, p, start, n)

        @pl.loop(0, n // 16)
        def _(g):
            here = pl.ds(pl.multiple_of(src.start + g * 16, 16), 16)
            pieces = [sent[j, here, :] for j in range(n_row)]
            for i in range(n_row):
                value = pick(p, i, pieces).astype(jnp.float32)
                sent[i, here, :] = (value * factor[p * n_row + i]).astype(sent.dtype)

    back = peer_row(n_row - half) * ratio

    def begin_mini(h):
        src, dst = rows_of(h, 1, 0, mini)
        for t, s in enumerate(near):
            to = peer_row(s)

            @pl.when(mine + h == col)
            def _():
                remote(sent.at[to, src], got_ref.at[col, dst], send1, mini1.at[h, s - 1], to, col).start()

            @pl.when(mine + h != col)
            def _():
                if h == 0 and t == 0:
                    remote(sent.at[to, src], relay.at[col], send1, relay_sems.at[0], row, mine).start()
                else:
                    remote(sent.at[to, src], mid.at[n_row - 1 - s, src], send1, mini1.at[h, s - 1], to, col).start()
        start_second(0, h, 1, 0, mini, 1, 1)

    def forward_mini(h):
        src, _ = rows_of(h, 1, 0, mini)
        for t, s in enumerate(close):
            block = mid.at[n_row - 1 - s, src]
            if h == 0 and t == 0:
                @pl.when(back == col)
                def _():
                    wait_bytes(block, mini1.at[h, s - 1])
            else:
                wait_bytes(block, mini1.at[h, s - 1])
                start_second(s, h, 1, 0, mini, 1, 1)

    late = list(range(held, len(heads)))
    base = 0
    for p, (start, size, count) in enumerate(bodies):
        def place(k, start=start, size=size):
            return lax.rem(k, ratio), start + (k // ratio) * size

        def prepare(k, p=p, size=size, place=place):
            h, at = place(k)
            prepare_rows(h, p, at, size)

        def begin(k, p=p, size=size, base=base, place=place):
            h, at = place(k)
            start_first(lambda s: body1.at[base + k], h, p, at, size)
            start_second(0, h, p, at, size, 1)

        def forward(k, p=p, size=size, base=base, place=place):
            h, at = place(k)
            src, _ = rows_of(h, p, at, size)
            wait_bytes(mid.at[:, src], body1.at[base + k])
            for s in far:
                start_second(s, h, p, at, size, 1)

        steps = count * ratio
        if p == 0:
            for h in range(ratio):
                prepare_rows(h, 1, 0, mini)
        prepare(0)
        if p == 0:
            for h in range(ratio):
                begin_mini(h)
            for s in range(1, n_col):
                remote(
                    total.at[row], peak_all.at[col], peak_send.at[1], peak_recv.at[1], row, peer_col(s)
                ).start()
            peak_all[col] = total[row]
        prepare(1)
        begin(0)
        for e in late:
            forward_head(e)
        if p == 0:
            for h in range(ratio):
                forward_mini(h)
        late = []

        @pl.loop(1, steps + LAG)
        def _(k, steps=steps, prepare=prepare, begin=begin, forward=forward):
            @pl.when(k + 1 < steps)
            def _():
                prepare(k + 1)

            @pl.when(k < steps)
            def _():
                begin(k)

            @pl.when(k >= LAG)
            def _():
                forward(k - LAG)

        base += steps

    others = pl.ds(0, n_col - 1)

    @pl.when(mine == col)
    def _():
        wait_bytes(relay.at[others], relay_sems.at[0])
        _, dst = rows_of(0, 1, 0, mini)
        for s in range(1, n_col):
            other = peer_col(s)
            remote(
                relay.at[other], got_ref.at[other, dst], relay_sems.at[1], recv2.at[1], peer_row(half), col
            ).start()

    wait_bytes(peak_all.at[others], peak_send.at[1])
    wait_bytes(peak_all.at[others], peak_recv.at[1])
    wait_bytes(got_ref.at[others, pl.ds(0, raw)], recv2.at[0])
    for c in range(n_col):
        base_peak = peak_all[c] + EPSILON
        scales_ref[:, pl.ds(c * piece, piece)] = base_peak / LIMIT
        value = (LIMIT / base_peak)[0:1]

        @pl.loop(0, raw // 16)
        def _(g):
            here = pl.ds(pl.multiple_of(g * 16, 16), 16)
            got_ref[c, here, :] = (got_ref[c, here, :].astype(jnp.float32) * value).astype(got_ref.dtype)

    wait_bytes(peak_mid, peak_send.at[0])
    wait_bytes(mid, send1)
    wait_bytes(got_ref.at[others, pl.ds(0, 2 * depth - mini)], send2.at[0])

    @pl.when(back == col)
    def _():
        wait_bytes(sent.at[0, pl.ds(0, (n_row * ratio - 1) * mini)], send2.at[1])

    @pl.when(back != col)
    def _():
        wait_bytes(sent.at[0, pl.ds(0, (n_row * ratio - 2) * mini)], send2.at[1])

    @pl.when(mine == col)
    def _():
        wait_bytes(relay.at[others], relay_sems.at[1])

    wait_bytes(got_ref.at[others, pl.ds(raw, 2 * depth - raw)], recv2.at[1])


def move_call(gate_weight, up_weight, routes, n_row, n_col):
    height, width = gate_weight.shape
    kind = gate_weight.dtype
    piece = width // n_row
    ratio = n_col // n_row
    depth = height // ratio
    head = [(q, 16) for q in range(0, RAW, 16)]
    small = SMALL * 16
    large = (depth - MINI) // LARGE
    bodies = [(RAW, small, (depth - RAW) // small), (MINI, large, LARGE)]
    steps = sum(count for _, _, count in bodies) * ratio
    dma = pltpu.SemaphoreType.DMA
    return pl.pallas_call(
        functools.partial(move_kernel, n_row, n_col, depth, RAW, head, MINI, bodies),
        out_shape=[
            pltpu.VMEM((n_col, 2 * depth, piece), kind),
            pltpu.VMEM((2, n_col * piece), jnp.float32),
        ],
        in_specs=[pl.BlockSpec(memory_space=pl.ANY)] * 3,
        out_specs=[
            pl.BlockSpec(memory_space=pltpu.VMEM),
            pl.BlockSpec(memory_space=pltpu.VMEM),
        ],
        scratch_shapes=[
            pltpu.SMEM(routes.shape, routes.dtype),
            pltpu.VMEM((n_row, 2 * height, piece), kind),
            pltpu.VMEM((n_row - 1, 2 * height, piece), kind),
            pltpu.VMEM((n_col, MINI, piece), kind),
            pltpu.VMEM((2, 16, width), kind),
            pltpu.VMEM((n_row, 2, piece), jnp.float32),
            pltpu.VMEM((n_row - 1, n_row, 2, piece), jnp.float32),
            pltpu.VMEM((n_row, 2, piece), jnp.float32),
            pltpu.VMEM((2 * n_row, 1, piece), jnp.float32),
            pltpu.VMEM((n_col, 2, piece), jnp.float32),
            dma,
            dma((4 * ratio,)),
            dma,
            dma((len(head) * ratio, n_row - 1)),
            dma((ratio, n_row - 1)),
            dma((steps,)),
            dma((2,)),
            dma((2,)),
            dma((2,)),
            dma((2,)),
            dma((2,)),
        ],
        compiler_params=pltpu.CompilerParams(
            collective_id=0, has_side_effects=True, vmem_limit_bytes=MOVE_BYTES
        ),
    )(routes, gate_weight, up_weight)


def store_kernel(depth, piece, got_ref, scales_ref, gate_ref, up_ref, out_ref, sems):
    for c in range(got_ref.shape[0]):
        for p, ref in enumerate((gate_ref, up_ref)):
            block = got_ref.at[c, pl.ds(p * depth, depth)]
            pltpu.make_async_copy(block, ref.at[:, pl.ds(c * piece, piece)], sems.at[0]).start()
    scales = pltpu.make_async_copy(scales_ref, out_ref, sems.at[1])
    scales.start()
    pltpu.make_async_copy(got_ref, got_ref, sems.at[0]).wait()
    scales.wait()


def store_call(got, scales):
    n_col, double, piece = got.shape
    depth = double // 2
    any_spec = pl.BlockSpec(memory_space=pl.ANY)
    return pl.pallas_call(
        functools.partial(store_kernel, depth, piece),
        in_specs=[pl.BlockSpec(memory_space=pltpu.VMEM), pl.BlockSpec(memory_space=pltpu.VMEM)],
        out_specs=[any_spec] * 3,
        out_shape=[
            jax.ShapeDtypeStruct((depth, n_col * piece), got.dtype),
            jax.ShapeDtypeStruct((depth, n_col * piece), got.dtype),
            jax.ShapeDtypeStruct((2, n_col * piece), jnp.float32),
        ],
        scratch_shapes=[pltpu.SemaphoreType.DMA((2,))],
        compiler_params=pltpu.CompilerParams(vmem_limit_bytes=STORE_BYTES),
    )(got, scales)


def kernel_shards(n_row, n_col, gate_weight, up_weight, routes):
    got, scales = move_call(gate_weight, up_weight, routes, n_row, n_col)
    return tuple(store_call(got, scales))


def fits(n_row, n_col, height, width):
    if n_col % n_row or width % n_row or (width // n_row) % 128:
        return False
    ratio = n_col // n_row
    depth = height // ratio
    if ratio != 2 or n_row != 4 or height % ratio or (depth - MINI) % (LARGE * 16) or depth % 64 or (depth - RAW) % (SMALL * 16):
        return False
    held_bytes = ((2 * n_row - 1) * 2 * height + n_col * 2 * height // ratio) * (width // n_row) * 2
    return held_bytes < 60 * 1024 * 1024


def solution(mesh):
    n_row, n_col = mesh.shape["row"], mesh.shape["col"]

    def shards(gate_weight, up_weight, routes):
        if fits(n_row, n_col, *gate_weight.shape):
            return kernel_shards(n_row, n_col, gate_weight, up_weight, routes)
        return plain_shards(gate_weight, up_weight, routes)

    return jax.shard_map(
        shards,
        mesh=mesh,
        in_specs=(P("row", "col"), P("row", "col"), P()),
        out_specs=(P("col", "row"), P("col", "row"), P(None, "row")),
        check_vma=False,
    )
```
